32 devices in a mesh: dp: 8 (over y, x, core), sub: 4 (over z).
Axes of the slice: x: 2, y: 2, z: 4, core: 2. Of those that a mesh axis runs over, the one named last changes fastest.
Arguments:
- queries: float32 [2048, 1024], P(('dp', 'sub')), may hold values from -8 to 8
- passages: float32 [2048, 1024], P(('dp', 'sub')), may hold values from -8 to 8
- positives: int32 [2048], P(('dp', 'sub')), may hold values from 0 to 2047, each once
Outputs:
- losses: float32 [2048], P(('dp', 'sub'))
- query_grads: float32 [2048, 1024], P(('dp', 'sub'))
- passage_grads: float32 [2048, 1024], P(('dp', 'sub'))
The draws below stay inside these ranges and needn't reach their ends.
All inputs are finite; a program needn't handle non-finite values.
Results may differ from the reference program's by a relative error of at most 0.00185.
The reference program's roundings to bfloat16 on the way count: a program that leaves them out, or rounds other values in their place, can miss the bound.
Values may be sent and summed in bfloat16 or wider, within the bound.
A program may use at most 128 MiB of HBM per device.

```python
import math
import jax
import jax.numpy as jnp
from jax import lax

D = 1024
BATCH = 2048


def embedding_pair(key):
    base = jax.random.fold_in(key, 41)
    streams = jax.random.split(base, 2)
    spread = (0.115 / math.sqrt(D)) ** 0.5
    queries = spread * jax.random.normal(streams[0], (BATCH, D), jnp.float32)
    passages = spread * jax.random.normal(streams[1], (BATCH, D), jnp.float32)
    return (jnp.clip(queries, -8.0, 8.0), jnp.clip(passages, -8.0, 8.0))


def draw_queries(key, part):
    return embedding_pair(key)[0]


def draw_passages(key, part):
    return embedding_pair(key)[1]


def setup_inputs(seed: int = 0) -> dict:
    splits = jax.random.split(jax.random.key(seed), 4)
    queries = draw_queries(jax.random.fold_in(splits[3], 71), 0)
    passages = draw_passages(jax.random.fold_in(splits[3], 71), 0)
    positives = jax.random.permutation(splits[2], BATCH).astype(jnp.int32)
    return {"queries": queries, "passages": passages, "positives": positives}


logit_scale = 20.0


def widen(values):
    return lax.optimization_barrier(values.astype(jnp.bfloat16)).astype(jnp.float32)


def reference(queries, passages, positives):
    query_wide = widen(queries)
    passage_wide = widen(passages)
    height = math.gcd(BATCH, 512)
    column_ids = jnp.arange(BATCH, dtype=jnp.int32)
    query_blocks = query_wide.reshape(BATCH // height, height, D)
    target_blocks = positives.astype(jnp.int32).reshape(BATCH // height, height)

    def advance(running, inputs):
        block_queries, block_targets = inputs
        scores = jnp.dot(block_queries, passage_wide.T, preferred_element_type=jnp.float32) * logit_scale
        highest = jnp.max(scores, axis=1)
        log_norm = highest + jnp.log(jnp.sum(jnp.exp(scores - highest[:, None]), axis=1))
        onehot = (column_ids[None, :] == block_targets[:, None]).astype(jnp.float32)
        positive_score = jnp.sum(onehot * scores, axis=1)
        weights = widen((jnp.exp(scores - log_norm[:, None]) - onehot) * logit_scale)
        block_grads = jnp.dot(weights, passage_wide, preferred_element_type=jnp.float32)
        running = running + jnp.dot(weights.T, block_queries, preferred_element_type=jnp.float32)
        return running, (log_norm - positive_score, block_grads)

    passage_grads, (losses, query_grads) = lax.scan(
        advance, jnp.zeros((BATCH, D), jnp.float32), (query_blocks, target_blocks))
    return losses.reshape(BATCH), query_grads.reshape(BATCH, D), passage_grads
```

```python
import functools

import jax
import jax.numpy as jnp
from jax import lax
from jax.experimental import pallas as pl
from jax.experimental.pallas import tpu as pltpu
from jax.sharding import PartitionSpec as P

logit_scale = 20.0
MESH = pl.DeviceIdType.MESH
CHUNKS = 2


class Copies:
    def __init__(self, send_sems, recv_sems, some_device):
        self.send_sems, self.recv_sems, self.some_device = send_sems, recv_sems, some_device
        self.sent, self.numbers = [], {}

    def number(self, key):
        return self.numbers.setdefault(key, len(self.numbers))

    def send(self, key, src, dst, device):
        i = self.number(key)
        copy = pltpu.make_async_remote_copy(
            src_ref=src, dst_ref=dst, send_sem=self.send_sems.at[i], recv_sem=self.recv_sems.at[i],
            device_id=device, device_id_type=MESH)
        copy.start()
        self.sent.append(copy)

    def arrive(self, key, dst):
        i = self.number(key)
        pltpu.make_async_remote_copy(
            src_ref=dst, dst_ref=dst, send_sem=self.send_sems.at[i], recv_sem=self.recv_sems.at[i],
            device_id=self.some_device, device_id_type=MESH).wait_recv()

    def finish(self):
        for copy in self.sent:
            copy.wait_send()


def kernel(nd, ns, q_ref, p_ref, t_ref, loss_ref, qg_ref, pg_ref,
           qall, pall, tall, st, wt, w, stat_out, stat_in, qpart, qsend, qrecv,
           ppart, ppartner, psend, precv, send_sems, recv_sems):
    rows, width = q_ref.shape
    nh, nz = nd // 4, ns // 2
    chips = nh * nz
    dp, sub = lax.axis_index("dp"), lax.axis_index("sub")
    core, x, h = dp % 2, (dp // 2) % 2, dp // 4
    l, s = sub % 2, sub // 2

    def device(dx=0, dl=0, dh=0, ds=0, dc=0):
        there = ((h + dh) % nh) * 4 + ((x + dx) % 2) * 2 + (core + dc) % 2
        return (there, ((s + ds) % nz) * 2 + (l + dl) % 2)

    partner = device(dc=1)
    peers = [device(dx=a // 2, dl=a % 2) for a in range(1, 4)]
    peers += [device(dh=b % nh, ds=b // nh) for b in range(1, chips)] + [partner]
    barrier = pltpu.get_barrier_semaphore()
    for peer in peers:
        pl.semaphore_signal(barrier, inc=1, device_id=peer, device_id_type=MESH)
    qall[pl.ds(0, rows), :] = q_ref[...].astype(jnp.bfloat16)
    pall[pl.ds(0, rows), :] = p_ref[...].astype(jnp.bfloat16)
    tall[0] = t_ref[...]
    pl.semaphore_wait(barrier, len(peers))

    copies = Copies(send_sems, recv_sems, partner)
    piece = rows // CHUNKS

    def block(ref, slot, part=None):
        if part is None:
            return ref.at[pl.ds(slot * rows, rows), :]
        return ref.at[pl.ds(slot * rows + part * piece, piece), :]

    def pslot(dc, ds, dh):
        return (dc * nz + ds % nz) * nh + dh % nh

    def to_partner(ds, dh, part=None):
        copies.send(("pc", ds, dh, part), block(pall, pslot(0, ds, dh), part),
                    block(pall, pslot(1, ds, dh), part), partner)

    for part in range(CHUNKS):
        copies.send(("ql", part), block(qall, 0, part), block(qall, 1, part), device(dl=1))
    for ds in range(1, nz):
        for part in range(CHUNKS):
            copies.send(("ps", (-ds) % nz, part), block(pall, 0, part),
                        block(pall, pslot(0, -ds, 0), part), device(ds=ds))
    copies.send(("qx",), block(qall, 0), block(qall, 2), device(dx=1))
    for dh in range(1, nh):
        copies.send(("ph", (-dh) % nh), block(pall, 0), block(pall, pslot(0, 0, -dh)), device(dh=dh))
    to_partner(0, 0)
    for a in range(1, 4):
        copies.send(("t", a), tall.at[0], tall.at[a], device(dx=a // 2, dl=a % 2))

    for part in range(CHUNKS):
        copies.arrive(("ql", part), block(qall, 1, part))
        copies.send(("qd", part), block(qall, 1, part), block(qall, 3, part), device(dx=1))
    for dh in range(1, nh):
        copies.arrive(("ph", dh), block(pall, pslot(0, 0, dh)))
        to_partner(0, dh)
    for part in range(CHUNKS):
        for ds in range(1, nz):
            here = block(pall, pslot(0, ds, 0), part)
            copies.arrive(("ps", ds, part), here)
            for dh in range(1, nh):
                copies.send(("pd", ds, (-dh) % nh, part), here,
                            block(pall, pslot(0, ds, -dh), part), device(dh=dh))
            to_partner(ds, 0, part)
    copies.arrive(("qx",), block(qall, 2))
    for part in range(CHUNKS):
        copies.arrive(("qd", part), block(qall, 3, part))
    for a in range(1, 4):
        copies.arrive(("t", a), tall.at[a])

    targets = jnp.concatenate([tall[a] for a in range(4)], axis=1)
    queries = 4 * rows
    span = nh * rows
    stats = None

    def onehot_of(dc, ds):
        lines = lax.broadcasted_iota(jnp.int32, (rows, queries), 0)
        parts = []
        for dh in range(nh):
            there, along = device(dh=dh, ds=ds, dc=dc)
            parts.append(lines + (there * ns + along) * rows == targets)
        return parts

    def score(dc, ds, stats):
        base = (dc * nz + ds) * span
        for dh in range(0, nh, 2):
            count = min(2, nh - dh) * rows
            at = pl.ds(base + dh * rows, count)
            st[at, :] = logit_scale * lax.dot_general(
                pall[at, :], qall[...], (((1,), (1,)), ((), ())), preferred_element_type=jnp.float32)
        tile = st[pl.ds(base, span), :]
        top = jnp.max(tile, axis=0, keepdims=True)
        positive = jnp.zeros((1, queries), jnp.float32)
        for dh, hit in enumerate(onehot_of(dc, ds)):
            positive += jnp.sum(jnp.where(hit, tile[dh * rows:(dh + 1) * rows], 0.0), axis=0, keepdims=True)
        if stats is not None:
            top = jnp.maximum(top, stats[0])
        total = jnp.sum(jnp.exp(tile - top), axis=0, keepdims=True)
        if stats is not None:
            total += stats[1] * jnp.exp(stats[0] - top)
            positive += stats[2]
        return top, total, positive

    stats = score(0, 0, stats)
    for dh in range(nh):
        copies.arrive(("pc", 0, dh, None), block(pall, pslot(1, 0, dh)))
    stats = score(1, 0, stats)
    for ds in range(1, nz):
        for dh in range(1, nh):
            for part in range(CHUNKS):
                copies.arrive(("pd", ds, dh, part), block(pall, pslot(0, ds, dh), part))
            to_partner(ds, dh)
        stats = score(0, ds, stats)
        for part in range(CHUNKS):
            copies.arrive(("pc", ds, 0, part), block(pall, pslot(1, ds, 0), part))
        for dh in range(1, nh):
            copies.arrive(("pc", ds, dh, None), block(pall, pslot(1, ds, dh)))
        stats = score(1, ds, stats)

    stat_out[...] = jnp.concatenate(list(stats) + [jnp.zeros((5, queries), jnp.float32)], axis=0)
    for a in range(1, 4):
        copies.send(("s", a), stat_out, stat_in.at[a - 1], device(dx=a // 2, dl=a % 2))
    top, total, positive = stats
    for a in range(1, 4):
        copies.arrive(("s", a), stat_in.at[a - 1])
        theirs = stat_in[a - 1]
        halves = [theirs[:, :2 * rows], theirs[:, 2 * rows:]]
        if a // 2:
            halves.reverse()
        if a % 2:
            halves = [jnp.concatenate([v[:, rows:], v[:, :rows]], axis=1) for v in halves]
        theirs = jnp.concatenate(halves, axis=1)
        higher = jnp.maximum(top, theirs[0:1])
        total = total * jnp.exp(top - higher) + theirs[1:2] * jnp.exp(theirs[0:1] - higher)
        positive += theirs[2:3]
        top = higher
    log_norm = top + jnp.log(total)
    loss_ref[...] = (log_norm - positive)[:, :rows]

    for dc in range(2):
        for ds in range(nz):
            base = (dc * nz + ds) * span
            for dh, hit in enumerate(onehot_of(dc, ds)):
                at = pl.ds(base + dh * rows, rows)
                weights = (jnp.exp(st[at, :] - log_norm) - hit.astype(jnp.float32)) * logit_scale
                wt[at, :] = weights.astype(jnp.bfloat16)
    for i in range(2 * chips * rows // (2 * rows)):
        at = pl.ds(i * 2 * rows, 2 * rows)
        w[:, at] = wt[at, :].T

    step = 2 * rows
    half = chips * rows

    def passage_terms(first):
        for i in range(half // step):
            ppart[pl.ds(first + i * step, step), :] = jnp.dot(
                wt[pl.ds(first + i * step, step), :], qall[...], preferred_element_type=jnp.float32)

    passage_terms(half)
    copies.send(("pp",), ppart.at[pl.ds(half, half), :], ppartner, partner)
    for pair in (1, 0):
        at = pl.ds(pair * 2 * rows, 2 * rows)
        qpart[at, :] = jnp.dot(w[at, :], pall[...], preferred_element_type=jnp.float32)
        for a in (2 * pair + 1, 2 * pair):
            if a:
                qsend[a - 1] = qpart[pl.ds(a * rows, rows), :].astype(jnp.bfloat16)
                copies.send(("q", a), qsend.at[a - 1], qrecv.at[a - 1], device(dx=a // 2, dl=a % 2))
    passage_terms(0)
    copies.arrive(("pp",), ppartner)
    for ds in reversed(range(nz)):
        for dh in reversed(range(nh)):
            b = ds * nh + dh
            if b:
                at = pl.ds(b * rows, rows)
                psend[b - 1] = (ppart[at, :] + ppartner[at, :]).astype(jnp.bfloat16)
                back = ((-ds) % nz) * nh + (-dh) % nh
                copies.send(("p", back), psend.at[b - 1], precv.at[back - 1], device(dh=dh, ds=ds))
    grads = qpart[pl.ds(0, rows), :]
    for a in range(1, 4):
        copies.arrive(("q", a), qrecv.at[a - 1])
        grads += qrecv[a - 1].astype(jnp.float32)
    qg_ref[...] = grads
    grads = ppart[pl.ds(0, rows), :] + ppartner[pl.ds(0, rows), :]
    for b in range(1, chips):
        copies.arrive(("p", b), precv.at[b - 1])
        grads += precv[b - 1].astype(jnp.float32)
    pg_ref[...] = grads
    copies.finish()


def body(nd, ns, queries, passages, positives):
    rows, width = queries.shape
    nh, nz = nd // 4, ns // 2
    chips = nh * nz
    half, cols = chips * rows, 2 * chips * rows
    bf16, f32 = jnp.bfloat16, jnp.float32
    copies = 16 + 4 * CHUNKS + chips * (3 + 3 * CHUNKS)
    losses, query_grads, passage_grads = pl.pallas_call(
        functools.partial(kernel, nd, ns),
        out_shape=(
            jax.ShapeDtypeStruct((1, rows), f32),
            jax.ShapeDtypeStruct((rows, width), f32),
            jax.ShapeDtypeStruct((rows, width), f32),
        ),
        in_specs=[pl.BlockSpec(memory_space=pltpu.VMEM)] * 3,
        out_specs=(pl.BlockSpec(memory_space=pltpu.VMEM),) * 3,
        scratch_shapes=[
            pltpu.VMEM((4 * rows, width), bf16),
            pltpu.VMEM((cols, width), bf16),
            pltpu.VMEM((4, 1, rows), jnp.int32),
            pltpu.VMEM((cols, 4 * rows), f32),
            pltpu.VMEM((cols, 4 * rows), bf16),
            pltpu.VMEM((4 * rows, cols), bf16),
            pltpu.VMEM((8, 4 * rows), f32),
            pltpu.VMEM((3, 8, 4 * rows), f32),
            pltpu.VMEM((4 * rows, width), f32),
            pltpu.VMEM((3, rows, width), bf16),
            pltpu.VMEM((3, rows, width), bf16),
            pltpu.VMEM((cols, width), f32),
            pltpu.VMEM((half, width), f32),
            pltpu.VMEM((chips - 1, rows, width), bf16),
            pltpu.VMEM((chips - 1, rows, width), bf16),
            pltpu.SemaphoreType.DMA((copies,)),
            pltpu.SemaphoreType.DMA((copies,)),
        ],
        compiler_params=pltpu.CompilerParams(
            collective_id=0, has_side_effects=True, vmem_limit_bytes=64 * 1024 * 1024 - 65536
        ),
    )(queries, passages, positives.reshape(1, rows))
    return losses.reshape(rows), query_grads, passage_grads


def solution(mesh):
    placed = (P(("dp", "sub"), None), P(("dp", "sub"), None), P(("dp", "sub")))
    return jax.shard_map(
        functools.partial(body, mesh.shape["dp"], mesh.shape["sub"]),
        mesh=mesh,
        in_specs=placed,
        out_specs=(P(("dp", "sub")), P(("dp", "sub"), None), P(("dp", "sub"), None)),
        check_vma=False,
    )
```

```python
import functools
import math

import jax
import jax.numpy as jnp
from jax import lax
from jax.experimental import pallas as pl
from jax.experimental.pallas import tpu as pltpu
from jax.sharding import PartitionSpec as P

logit_scale = 20.0
MESH = pl.DeviceIdType.MESH
CHUNKS = 4


class Copies:
    def __init__(self, send_sems, recv_sems, some_device):
        self.send_sems, self.recv_sems, self.some_device = send_sems, recv_sems, some_device
        self.sent, self.numbers = [], {}

    def number(self, key):
        return self.numbers.setdefault(key, len(self.numbers))

    def send(self, key, src, dst, device):
        i = self.number(key)
        copy = pltpu.make_async_remote_copy(
            src_ref=src, dst_ref=dst, send_sem=self.send_sems.at[i], recv_sem=self.recv_sems.at[i],
            device_id=device, device_id_type=MESH)
        copy.start()
        self.sent.append(copy)

    def arrive(self, key, dst):
        i = self.number(key)
        pltpu.make_async_remote_copy(
            src_ref=dst, dst_ref=dst, send_sem=self.send_sems.at[i], recv_sem=self.recv_sems.at[i],
            device_id=self.some_device, device_id_type=MESH).wait_recv()

    def finish(self):
        for copy in self.sent:
            copy.wait_send()


def kernel(nd, ns, q_ref, p_ref, t_ref, out_ref,
           qall, pall, tall, st, wt, w, stat_out, stat_in, qpart, qsend, qrecv,
           ppart, ppartner, pmid, psend, precv, send_sems, recv_sems):
    rows, width = q_ref.shape
    nh, nz = nd // 4, ns // 2
    chips = nh * nz
    dp, sub = lax.axis_index("dp"), lax.axis_index("sub")
    core, x, h = dp % 2, (dp // 2) % 2, dp // 4
    l, s = sub % 2, sub // 2

    def device(dx=0, dl=0, dh=0, ds=0, dc=0):
        there = ((h + dh) % nh) * 4 + ((x + dx) % 2) * 2 + (core + dc) % 2
        return (there, ((s + ds) % nz) * 2 + (l + dl) % 2)

    partner = device(dc=1)
    peers = [device(dx=1), device(dl=1), partner]
    peers += [device(dh=dh) for dh in range(1, nh)] + [device(ds=ds) for ds in range(1, nz)]
    barrier = pltpu.get_barrier_semaphore()
    for peer in peers:
        pl.semaphore_signal(barrier, inc=1, device_id=peer, device_id_type=MESH)
    qall[pl.ds(0, rows), :] = q_ref[...].astype(jnp.bfloat16)
    pall[pl.ds(0, rows), :] = p_ref[...].astype(jnp.bfloat16)
    tall[0] = t_ref[...]
    pl.semaphore_wait(barrier, len(peers))

    copies = Copies(send_sems, recv_sems, partner)
    piece = rows // CHUNKS

    def block(ref, slot, part=None):
        if part is None:
            return ref.at[pl.ds(slot * rows, rows), :]
        return ref.at[pl.ds(slot * rows + part * piece, piece), :]

    def pslot(dc, ds, dh):
        return (dc * nz + ds % nz) * nh + dh % nh

    def to_partner(ds, dh, part=None):
        copies.send(("pc", ds, dh, part), block(pall, pslot(0, ds, dh), part),
                    block(pall, pslot(1, ds, dh), part), partner)

    for part in range(CHUNKS):
        copies.send(("ql", part), block(qall, 0, part), block(qall, 1, part), device(dl=1))
    for ds in range(1, nz):
        for part in range(CHUNKS):
            copies.send(("ps", (-ds) % nz, part), block(pall, 0, part),
                        block(pall, pslot(0, -ds, 0), part), device(ds=ds))
    copies.send(("qx",), block(qall, 0), block(qall, 2), device(dx=1))
    for dh in range(1, nh):
        copies.send(("ph", (-dh) % nh), block(pall, 0), block(pall, pslot(0, 0, -dh)), device(dh=dh))
    to_partner(0, 0)
    copies.send(("t", 1), tall.at[0], tall.at[1], device(dl=1))
    copies.send(("t", 2), tall.at[0], tall.at[2], device(dx=1))

    for part in range(CHUNKS):
        copies.arrive(("ql", part), block(qall, 1, part))
        copies.send(("qd", part), block(qall, 1, part), block(qall, 3, part), device(dx=1))
    copies.arrive(("t", 1), tall.at[1])
    copies.send(("t", 3), tall.at[1], tall.at[3], device(dx=1))
    for dh in range(1, nh):
        copies.arrive(("ph", dh), block(pall, pslot(0, 0, dh)))
        to_partner(0, dh)
    for part in range(CHUNKS):
        for ds in range(1, nz):
            here = block(pall, pslot(0, ds, 0), part)
            copies.arrive(("ps", ds, part), here)
            for dh in range(1, nh):
                copies.send(("pd", ds, (-dh) % nh, part), here,
                            block(pall, pslot(0, ds, -dh), part), device(dh=dh))
            to_partner(ds, 0, part)
    copies.arrive(("qx",), block(qall, 2))
    for part in range(CHUNKS):
        copies.arrive(("qd", part), block(qall, 3, part))
    for a in range(2, 4):
        copies.arrive(("t", a), tall.at[a])

    targets = jnp.concatenate([tall[a] for a in range(4)], axis=1)
    queries = 4 * rows
    span = nh * rows
    stats = None

    def onehot_of(dc, ds):
        lines = lax.broadcasted_iota(jnp.int32, (rows, queries), 0)
        parts = []
        for dh in range(nh):
            there, along = device(dh=dh, ds=ds, dc=dc)
            parts.append(lines + (there * ns + along) * rows == targets)
        return parts

    def score(dc, ds, stats):
        base = (dc * nz + ds) * span
        for dh in range(0, nh, 2):
            count = min(2, nh - dh) * rows
            at = pl.ds(base + dh * rows, count)
            st[at, :] = logit_scale * lax.dot_general(
                pall[at, :], qall[...], (((1,), (1,)), ((), ())), preferred_element_type=jnp.float32)
        tile = st[pl.ds(base, span), :]
        top = jnp.max(tile, axis=0, keepdims=True)
        positive = jnp.zeros((1, queries), jnp.float32)
        for dh, hit in enumerate(onehot_of(dc, ds)):
            positive += jnp.sum(jnp.where(hit, tile[dh * rows:(dh + 1) * rows], 0.0), axis=0, keepdims=True)
        if stats is not None:
            top = jnp.maximum(top, stats[0])
        total = jnp.sum(jnp.exp(tile - top), axis=0, keepdims=True)
        if stats is not None:
            total += stats[1] * jnp.exp(stats[0] - top)
            positive += stats[2]
        return top, total, positive

    stats = score(0, 0, stats)
    for dh in range(nh):
        copies.arrive(("pc", 0, dh, None), block(pall, pslot(1, 0, dh)))
    stats = score(1, 0, stats)
    for ds in range(1, nz):
        for dh in range(1, nh):
            for part in range(CHUNKS):
                copies.arrive(("pd", ds, dh, part), block(pall, pslot(0, ds, dh), part))
            to_partner(ds, dh)
        stats = score(0, ds, stats)
        for part in range(CHUNKS):
            copies.arrive(("pc", ds, 0, part), block(pall, pslot(1, ds, 0), part))
        for dh in range(1, nh):
            copies.arrive(("pc", ds, dh, None), block(pall, pslot(1, ds, dh)))
        stats = score(1, ds, stats)

    stat_out[...] = jnp.concatenate(list(stats) + [jnp.zeros((5, queries), jnp.float32)], axis=0)
    for a in range(1, 4):
        copies.send(("s", a), stat_out, stat_in.at[a - 1], device(dx=a // 2, dl=a % 2))
    top, total, positive = stats
    for a in range(1, 4):
        copies.arrive(("s", a), stat_in.at[a - 1])
        theirs = stat_in[a - 1]
        halves = [theirs[:, :2 * rows], theirs[:, 2 * rows:]]
        if a // 2:
            halves.reverse()
        if a % 2:
            halves = [jnp.concatenate([v[:, rows:], v[:, :rows]], axis=1) for v in halves]
        theirs = jnp.concatenate(halves, axis=1)
        higher = jnp.maximum(top, theirs[0:1])
        total = total * jnp.exp(top - higher) + theirs[1:2] * jnp.exp(theirs[0:1] - higher)
        positive += theirs[2:3]
        top = higher
    log_norm = top + jnp.log(total)
    out_ref[pl.ds(2 * rows, 1), pl.ds(0, rows)] = (log_norm - positive)[:, :rows]

    for dc in range(2):
        for ds in range(nz):
            base = (dc * nz + ds) * span
            for dh, hit in enumerate(onehot_of(dc, ds)):
                at = pl.ds(base + dh * rows, rows)
                weights = (jnp.exp(st[at, :] - log_norm) - hit.astype(jnp.float32)) * logit_scale
                wt[at, :] = weights.astype(jnp.bfloat16)
    for i in range(2 * chips * rows // (2 * rows)):
        at = pl.ds(i * 2 * rows, 2 * rows)
        w[:, at] = wt[at, :].T

    step = 2 * rows
    half = chips * rows

    def passage_terms(dc, ds):
        first = dc * half + ds * span
        for i in range(-(-span // step)):
            at = pl.ds(first + i * step, min(step, span - i * step))
            ppart[at, :] = jnp.dot(wt[at, :], qall[...], preferred_element_type=jnp.float32)
        if dc:
            for dh in reversed(range(nh)):
                b = ds * nh + dh
                copies.send(("pp", b), block(ppart, chips + b), block(ppartner, b), partner)

    def both_cores(ds, dh):
        b = ds * nh + dh
        copies.arrive(("pp", b), block(ppartner, b))
        at = pl.ds(b * rows, rows)
        return at, ppart[at, :] + ppartner[at, :]

    def query_terms(pair):
        at = pl.ds(pair * 2 * rows, 2 * rows)
        qpart[at, :] = jnp.dot(w[at, :], pall[...], preferred_element_type=jnp.float32)
        for a in (2 * pair + 1, 2 * pair):
            if a:
                qsend[a - 1] = qpart[pl.ds(a * rows, rows), :].astype(jnp.bfloat16)
                copies.send(("q", a), qsend.at[a - 1], qrecv.at[a - 1], device(dx=a // 2, dl=a % 2))

    for ds in reversed(range(1, nz)):
        passage_terms(1, ds)
        passage_terms(0, ds)
    query_terms(1)
    for ds in reversed(range(1, nz)):
        for dh in reversed(range(1, nh)):
            at, both = both_cores(ds, dh)
            ppart[at, :] = both
            for part in range(CHUNKS):
                here = ((ds - 1) * (nh - 1) + nh - dh - 1)
                copies.send(("pm", ds, nh - dh, part), block(ppart, ds * nh + dh, part),
                            block(pmid, here, part), device(dh=dh))
    passage_terms(1, 0)
    passage_terms(0, 0)
    query_terms(0)
    for dh in reversed(range(1, nh)):
        at, both = both_cores(0, dh)
        psend[pl.ds((dh - 1) * rows, rows), :] = both.astype(jnp.bfloat16)
        copies.send(("p", nh - dh), block(psend, dh - 1), block(precv, nh - dh - 1), device(dh=dh))
    for ds in range(1, nz):
        at, both = both_cores(ds, 0)
        ppart[at, :] = both
        for part in range(CHUNKS):
            total = ppart[pl.ds(ds * span + part * piece, piece), :]
            for dh in range(1, nh):
                here = (ds - 1) * (nh - 1) + dh - 1
                copies.arrive(("pm", ds, dh, part), block(pmid, here, part))
                total += pmid[pl.ds(here * rows + part * piece, piece), :]
            slot = nh - 2 + ds
            psend[pl.ds(slot * rows + part * piece, piece), :] = total.astype(jnp.bfloat16)
            copies.send(("pz", nz - ds, part), block(psend, slot, part),
                        block(precv, nh - 2 + nz - ds, part), device(ds=ds))
    grads = qpart[pl.ds(0, rows), :]
    for a in range(1, 4):
        copies.arrive(("q", a), qrecv.at[a - 1])
        grads += qrecv[a - 1].astype(jnp.float32)
    out_ref[pl.ds(0, rows), :] = grads
    at, grads = both_cores(0, 0)
    for dh in range(1, nh):
        copies.arrive(("p", dh), block(precv, dh - 1))
        grads += precv[pl.ds((dh - 1) * rows, rows), :].astype(jnp.float32)
    ppart[at, :] = grads
    for part in range(CHUNKS):
        grads = ppart[pl.ds(part * piece, piece), :]
        for ds in range(1, nz):
            copies.arrive(("pz", ds, part), block(precv, nh - 2 + ds, part))
            at = pl.ds((nh - 2 + ds) * rows + part * piece, piece)
            grads += precv[at, :].astype(jnp.float32)
        out_ref[pl.ds(rows + part * piece, piece), :] = grads
    copies.finish()


def unpack(packed_ref, loss_ref, qg_ref, pg_ref):
    rows = qg_ref.shape[0]
    loss_ref[...] = packed_ref[pl.ds(2 * rows, 1), pl.ds(0, rows)]
    qg_ref[...] = packed_ref[pl.ds(0, rows), :]
    pg_ref[...] = packed_ref[pl.ds(rows, rows), :]


def body(nd, ns, queries, passages, positives):
    rows, width = queries.shape
    nh, nz = nd // 4, ns // 2
    chips = nh * nz
    half, cols = chips * rows, 2 * chips * rows
    bf16, f32 = jnp.bfloat16, jnp.float32
    copies = 16 + 5 * CHUNKS + chips * (3 + 4 * CHUNKS)
    scratch = [
        ((4 * rows, width), bf16),
        ((cols, width), bf16),
        ((4, 1, rows), jnp.int32),
        ((cols, 4 * rows), f32),
        ((cols, 4 * rows), bf16),
        ((4 * rows, cols), bf16),
        ((8, 4 * rows), f32),
        ((3, 8, 4 * rows), f32),
        ((4 * rows, width), f32),
        ((3, rows, width), bf16),
        ((3, rows, width), bf16),
        ((cols, width), f32),
        ((half, width), f32),
        ((max(1, (nz - 1) * (nh - 1)) * rows, width), f32),
        ((max(1, nz + nh - 2) * rows, width), bf16),
        ((max(1, nz + nh - 2) * rows, width), bf16),
    ]
    held = sum(math.prod(shape) * jnp.dtype(kind).itemsize for shape, kind in scratch)
    vmem = pl.BlockSpec(memory_space=pltpu.VMEM)
    packed = pl.pallas_call(
        functools.partial(kernel, nd, ns),
        out_shape=jax.ShapeDtypeStruct((2 * rows + 8, width), f32),
        in_specs=[vmem] * 3,
        out_specs=vmem,
        scratch_shapes=[pltpu.VMEM(*entry) for entry in scratch] + [
            pltpu.SemaphoreType.DMA((copies,)),
            pltpu.SemaphoreType.DMA((copies,)),
        ],
        compiler_params=pltpu.CompilerParams(
            collective_id=0, has_side_effects=True, vmem_limit_bytes=held + 8 * 1024 * 1024
        ),
    )(queries, passages, positives.reshape(1, rows))
    losses, query_grads, passage_grads = pl.pallas_call(
        unpack,
        out_shape=(
            jax.ShapeDtypeStruct((1, rows), f32),
            jax.ShapeDtypeStruct((rows, width), f32),
            jax.ShapeDtypeStruct((rows, width), f32),
        ),
        in_specs=[vmem],
        out_specs=(vmem,) * 3,
        compiler_params=pltpu.CompilerParams(vmem_limit_bytes=8 * 1024 * 1024),
    )(packed)
    return losses.reshape(rows), query_grads, passage_grads


def solution(mesh):
    placed = (P(("dp", "sub"), None), P(("dp", "sub"), None), P(("dp", "sub")))
    return jax.shard_map(
        functools.partial(body, mesh.shape["dp"], mesh.shape["sub"]),
        mesh=mesh,
        in_specs=placed,
        out_specs=(P(("dp", "sub")), P(("dp", "sub"), None), P(("dp", "sub"), None)),
        check_vma=False,
    )
```

```python
import functools

import jax
import jax.numpy as jnp
from jax import lax
from jax.experimental import pallas as pl
from jax.experimental.pallas import tpu as pltpu
from jax.sharding import PartitionSpec as P

logit_scale = 20.0
MESH = pl.DeviceIdType.MESH
CHUNKS = 2


class Copies:
    def __init__(self, send_sems, recv_sems, some_device):
        self.send_sems, self.recv_sems, self.some_device = send_sems, recv_sems, some_device
        self.sent, self.numbers = [], {}

    def number(self, key):
        return self.numbers.setdefault(key, len(self.numbers))

    def send(self, key, src, dst, device):
        i = self.number(key)
        copy = pltpu.make_async_remote_copy(
            src_ref=src, dst_ref=dst, send_sem=self.send_sems.at[i], recv_sem=self.recv_sems.at[i],
            device_id=device, device_id_type=MESH)
        copy.start()
        self.sent.append(copy)

    def arrive(self, key, dst):
        i = self.number(key)
        pltpu.make_async_remote_copy(
            src_ref=dst, dst_ref=dst, send_sem=self.send_sems.at[i], recv_sem=self.recv_sems.at[i],
            device_id=self.some_device, device_id_type=MESH).wait_recv()

    def finish(self):
        for copy in self.sent:
            copy.wait_send()


def kernel(nd, ns, q_ref, p_ref, t_ref, out_ref,
           qin, pin, qall, pall, tall, st, wt, w, stat_out, stat_in, qpart, qsend, qrecv,
           ppart, ppartner, pmid, psend, precv, load_sems, send_sems, recv_sems):
    rows, width = q_ref.shape
    nh, nz = nd // 4, ns // 2
    chips = nh * nz
    dp, sub = lax.axis_index("dp"), lax.axis_index("sub")
    core, x, h = dp % 2, (dp // 2) % 2, dp // 4
    l, s = sub % 2, sub // 2

    def device(dx=0, dl=0, dh=0, ds=0, dc=0):
        there = ((h + dh) % nh) * 4 + ((x + dx) % 2) * 2 + (core + dc) % 2
        return (there, ((s + ds) % nz) * 2 + (l + dl) % 2)

    loads = [pltpu.make_async_copy(src, dst, load_sems.at[i])
             for i, (src, dst) in enumerate(((q_ref, qin), (p_ref, pin), (t_ref, tall.at[0])))]
    for load in loads:
        load.start()
    partner = device(dc=1)
    peers = [device(dx=1), device(dl=1), partner]
    peers += [device(dh=dh) for dh in range(1, nh)] + [device(ds=ds) for ds in range(1, nz)]
    barrier = pltpu.get_barrier_semaphore()
    for peer in peers:
        pl.semaphore_signal(barrier, inc=1, device_id=peer, device_id_type=MESH)
    loads[0].wait()
    qall[pl.ds(0, rows), :] = qin[...].astype(jnp.bfloat16)
    loads[1].wait()
    pall[pl.ds(0, rows), :] = pin[...].astype(jnp.bfloat16)
    loads[2].wait()
    pl.semaphore_wait(barrier, len(peers))

    copies = Copies(send_sems, recv_sems, partner)
    piece = rows // CHUNKS

    def block(ref, slot, part=None):
        if part is None:
            return ref.at[pl.ds(slot * rows, rows), :]
        return ref.at[pl.ds(slot * rows + part * piece, piece), :]

    def pslot(dc, ds, dh):
        return (dc * nz + ds % nz) * nh + dh % nh

    def to_partner(ds, dh, part=None):
        copies.send(("pc", ds, dh, part), block(pall, pslot(0, ds, dh), part),
                    block(pall, pslot(1, ds, dh), part), partner)

    for part in range(CHUNKS):
        copies.send(("ql", part), block(qall, 0, part), block(qall, 1, part), device(dl=1))
    for ds in range(1, nz):
        for part in range(CHUNKS):
            copies.send(("ps", (-ds) % nz, part), block(pall, 0, part),
                        block(pall, pslot(0, -ds, 0), part), device(ds=ds))
    copies.send(("qx",), block(qall, 0), block(qall, 2), device(dx=1))
    for dh in range(1, nh):
        copies.send(("ph", (-dh) % nh), block(pall, 0), block(pall, pslot(0, 0, -dh)), device(dh=dh))
    to_partner(0, 0)
    copies.send(("t", 1), tall.at[0], tall.at[1], device(dl=1))
    copies.send(("t", 2), tall.at[0], tall.at[2], device(dx=1))

    for part in range(CHUNKS):
        copies.arrive(("ql", part), block(qall, 1, part))
        copies.send(("qd", part), block(qall, 1, part), block(qall, 3, part), device(dx=1))
    copies.arrive(("t", 1), tall.at[1])
    copies.send(("t", 3), tall.at[1], tall.at[3], device(dx=1))
    for dh in range(1, nh):
        copies.arrive(("ph", dh), block(pall, pslot(0, 0, dh)))
        to_partner(0, dh)
    for part in range(CHUNKS):
        for ds in range(1, nz):
            here = block(pall, pslot(0, ds, 0), part)
            copies.arrive(("ps", ds, part), here)
            for dh in range(1, nh):
                copies.send(("pd", ds, (-dh) % nh, part), here,
                            block(pall, pslot(0, ds, -dh), part), device(dh=dh))
            to_partner(ds, 0, part)
    copies.arrive(("qx",), block(qall, 2))
    for part in range(CHUNKS):
        copies.arrive(("qd", part), block(qall, 3, part))
    for a in range(2, 4):
        copies.arrive(("t", a), tall.at[a])

    targets = jnp.concatenate([tall[a] for a in range(4)], axis=1)
    queries = 4 * rows
    span = nh * rows
    stats = None

    def onehot_of(dc, ds):
        lines = lax.broadcasted_iota(jnp.int32, (rows, queries), 0)
        parts = []
        for dh in range(nh):
            there, along = device(dh=dh, ds=ds, dc=dc)
            parts.append(lines + (there * ns + along) * rows == targets)
        return parts

    def score(dc, ds, stats):
        base = (dc * nz + ds) * span
        for dh in range(0, nh, 2):
            count = min(2, nh - dh) * rows
            at = pl.ds(base + dh * rows, count)
            st[at, :] = logit_scale * lax.dot_general(
                pall[at, :], qall[...], (((1,), (1,)), ((), ())), preferred_element_type=jnp.float32)
        tile = st[pl.ds(base, span), :]
        top = jnp.max(tile, axis=0, keepdims=True)
        positive = jnp.zeros((1, queries), jnp.float32)
        for dh, hit in enumerate(onehot_of(dc, ds)):
            positive += jnp.sum(jnp.where(hit, tile[dh * rows:(dh + 1) * rows], 0.0), axis=0, keepdims=True)
        if stats is not None:
            top = jnp.maximum(top, stats[0])
        total = jnp.sum(jnp.exp(tile - top), axis=0, keepdims=True)
        if stats is not None:
            total += stats[1] * jnp.exp(stats[0] - top)
            positive += stats[2]
        return top, total, positive

    stats = score(0, 0, stats)
    for dh in range(nh):
        copies.arrive(("pc", 0, dh, None), block(pall, pslot(1, 0, dh)))
    stats = score(1, 0, stats)
    for ds in range(1, nz):
        for dh in range(1, nh):
            for part in range(CHUNKS):
                copies.arrive(("pd", ds, dh, part), block(pall, pslot(0, ds, dh), part))
            to_partner(ds, dh)
        stats = score(0, ds, stats)
        for part in range(CHUNKS):
            copies.arrive(("pc", ds, 0, part), block(pall, pslot(1, ds, 0), part))
        for dh in range(1, nh):
            copies.arrive(("pc", ds, dh, None), block(pall, pslot(1, ds, dh)))
        stats = score(1, ds, stats)

    stat_out[...] = jnp.concatenate(list(stats) + [jnp.zeros((5, queries), jnp.float32)], axis=0)
    for a in range(1, 4):
        copies.send(("s", a), stat_out, stat_in.at[a - 1], device(dx=a // 2, dl=a % 2))
    top, total, positive = stats
    for a in range(1, 4):
        copies.arrive(("s", a), stat_in.at[a - 1])
        theirs = stat_in[a - 1]
        halves = [theirs[:, :2 * rows], theirs[:, 2 * rows:]]
        if a // 2:
            halves.reverse()
        if a % 2:
            halves = [jnp.concatenate([v[:, rows:], v[:, :rows]], axis=1) for v in halves]
        theirs = jnp.concatenate(halves, axis=1)
        higher = jnp.maximum(top, theirs[0:1])
        total = total * jnp.exp(top - higher) + theirs[1:2] * jnp.exp(theirs[0:1] - higher)
        positive += theirs[2:3]
        top = higher
    log_norm = top + jnp.log(total)
    out_ref[pl.ds(2 * rows, 1), pl.ds(0, rows)] = (log_norm - positive)[:, :rows]

    for dc in range(2):
        for ds in range(nz):
            base = (dc * nz + ds) * span
            for dh, hit in enumerate(onehot_of(dc, ds)):
                at = pl.ds(base + dh * rows, rows)
                weights = (jnp.exp(st[at, :] - log_norm) - hit.astype(jnp.float32)) * logit_scale
                wt[at, :] = weights.astype(jnp.bfloat16)
    for i in range(2 * chips * rows // (2 * rows)):
        at = pl.ds(i * 2 * rows, 2 * rows)
        w[:, at] = wt[at, :].T

    step = 2 * rows
    half = chips * rows

    def passage_terms(dc, ds):
        first = dc * half + ds * span
        for i in range(-(-span // step)):
            at = pl.ds(first + i * step, min(step, span - i * step))
            ppart[at, :] = jnp.dot(wt[at, :], qall[...], preferred_element_type=jnp.float32)
        if dc:
            for dh in reversed(range(nh)):
                b = ds * nh + dh
                copies.send(("pp", b), block(ppart, chips + b), block(ppartner, b), partner)

    def both_cores(ds, dh):
        b = ds * nh + dh
        copies.arrive(("pp", b), block(ppartner, b))
        at = pl.ds(b * rows, rows)
        return at, ppart[at, :] + ppartner[at, :]

    def query_terms(pair):
        at = pl.ds(pair * 2 * rows, 2 * rows)
        qpart[at, :] = jnp.dot(w[at, :], pall[...], preferred_element_type=jnp.float32)
        for a in (2 * pair + 1, 2 * pair):
            if a:
                qsend[a - 1] = qpart[pl.ds(a * rows, rows), :].astype(jnp.bfloat16)
                copies.send(("q", a), qsend.at[a - 1], qrecv.at[a - 1], device(dx=a // 2, dl=a % 2))

    for ds in reversed(range(1, nz)):
        passage_terms(1, ds)
        passage_terms(0, ds)
    query_terms(1)
    for ds in reversed(range(1, nz)):
        for dh in reversed(range(1, nh)):
            at, both = both_cores(ds, dh)
            ppart[at, :] = both
            for part in range(CHUNKS):
                here = ((ds - 1) * (nh - 1) + nh - dh - 1)
                copies.send(("pm", ds, nh - dh, part), block(ppart, ds * nh + dh, part),
                            block(pmid, here, part), device(dh=dh))
    passage_terms(1, 0)
    passage_terms(0, 0)
    query_terms(0)
    for dh in reversed(range(1, nh)):
        at, both = both_cores(0, dh)
        psend[pl.ds((dh - 1) * rows, rows), :] = both.astype(jnp.bfloat16)
        copies.send(("p", nh - dh), block(psend, dh - 1), block(precv, nh - dh - 1), device(dh=dh))
    for ds in range(1, nz):
        at, both = both_cores(ds, 0)
        ppart[at, :] = both
        for part in range(CHUNKS):
            total = ppart[pl.ds(ds * span + part * piece, piece), :]
            for dh in range(1, nh):
                here = (ds - 1) * (nh - 1) + dh - 1
                copies.arrive(("pm", ds, dh, part), block(pmid, here, part))
                total += pmid[pl.ds(here * rows + part * piece, piece), :]
            slot = nh - 2 + ds
            psend[pl.ds(slot * rows + part * piece, piece), :] = total.astype(jnp.bfloat16)
            copies.send(("pz", nz - ds, part), block(psend, slot, part),
                        block(precv, nh - 2 + nz - ds, part), device(ds=ds))
    grads = qpart[pl.ds(0, rows), :]
    for a in range(1, 4):
        copies.arrive(("q", a), qrecv.at[a - 1])
        grads += qrecv[a - 1].astype(jnp.float32)
    out_ref[pl.ds(0, rows), :] = grads
    at, grads = both_cores(0, 0)
    for dh in range(1, nh):
        copies.arrive(("p", dh), block(precv, dh - 1))
        grads += precv[pl.ds((dh - 1) * rows, rows), :].astype(jnp.float32)
    ppart[at, :] = grads
    for part in range(CHUNKS):
        grads = ppart[pl.ds(part * piece, piece), :]
        for ds in range(1, nz):
            copies.arrive(("pz", ds, part), block(precv, nh - 2 + ds, part))
            at = pl.ds((nh - 2 + ds) * rows + part * piece, piece)
            grads += precv[at, :].astype(jnp.float32)
        out_ref[pl.ds(rows + part * piece, piece), :] = grads
    copies.finish()


def unpack(packed_ref, loss_ref, qg_ref, pg_ref):
    rows = qg_ref.shape[0]
    loss_ref[...] = packed_ref[pl.ds(2 * rows, 1), pl.ds(0, rows)]
    qg_ref[...] = packed_ref[pl.ds(0, rows), :]
    pg_ref[...] = packed_ref[pl.ds(rows, rows), :]


def body(nd, ns, queries, passages, positives):
    rows, width = queries.shape
    nh, nz = nd // 4, ns // 2
    chips = nh * nz
    half, cols = chips * rows, 2 * chips * rows
    bf16, f32 = jnp.bfloat16, jnp.float32
    copies = 16 + 5 * CHUNKS + chips * (3 + 4 * CHUNKS)
    scratch = [
        ((rows, width), f32),
        ((rows, width), f32),
        ((4 * rows, width), bf16),
        ((cols, width), bf16),
        ((4, 1, rows), jnp.int32),
        ((cols, 4 * rows), f32),
        ((cols, 4 * rows), bf16),
        ((4 * rows, cols), bf16),
        ((8, 4 * rows), f32),
        ((3, 8, 4 * rows), f32),
        ((4 * rows, width), f32),
        ((3, rows, width), bf16),
        ((3, rows, width), bf16),
        ((cols, width), f32),
        ((half, width), f32),
        ((max(1, (nz - 1) * (nh - 1)) * rows, width), f32),
        ((max(1, nz + nh - 2) * rows, width), bf16),
        ((max(1, nz + nh - 2) * rows, width), bf16),
    ]
    vmem = pl.BlockSpec(memory_space=pltpu.VMEM)
    packed = pl.pallas_call(
        functools.partial(kernel, nd, ns),
        out_shape=jax.ShapeDtypeStruct((2 * rows + 8, width), f32),
        in_specs=[pl.BlockSpec(memory_space=pl.ANY)] * 3,
        out_specs=vmem,
        scratch_shapes=[pltpu.VMEM(*entry) for entry in scratch] + [
            pltpu.SemaphoreType.DMA((3,)),
            pltpu.SemaphoreType.DMA((copies,)),
            pltpu.SemaphoreType.DMA((copies,)),
        ],
        compiler_params=pltpu.CompilerParams(
            collective_id=0, has_side_effects=True, vmem_limit_bytes=64 * 1024 * 1024 - 65536
        ),
    )(queries, passages, positives.reshape(1, rows))
    losses, query_grads, passage_grads = pl.pallas_call(
        unpack,
        out_shape=(
            jax.ShapeDtypeStruct((1, rows), f32),
            jax.ShapeDtypeStruct((rows, width), f32),
            jax.ShapeDtypeStruct((rows, width), f32),
        ),
        in_specs=[vmem],
        out_specs=(vmem,) * 3,
        compiler_params=pltpu.CompilerParams(vmem_limit_bytes=64 * 1024 * 1024 - 65536),
    )(packed)
    return losses.reshape(rows), query_grads, passage_grads


def solution(mesh):
    placed = (P(("dp", "sub"), None), P(("dp", "sub"), None), P(("dp", "sub")))
    return jax.shard_map(
        functools.partial(body, mesh.shape["dp"], mesh.shape["sub"]),
        mesh=mesh,
        in_specs=placed,
        out_specs=(P(("dp", "sub")), P(("dp", "sub"), None), P(("dp", "sub"), None)),
        check_vma=False,
    )
```
